256 devices in a mesh: gx: 4 (over x), gy: 4 (over y), gz: 16 (over z, core).
Axes of the slice: x: 4, y: 4, z: 8, core: 2. Of those that a mesh axis runs over, the one named last changes fastest.
Arguments:
- embeds: bfloat16 [2048, 128, 2048], P(('gx', 'gy', 'gz')), may hold values from -6 to 6
- dest_device: int32 [2048], P(('gx', 'gy', 'gz')), may hold values from 0 to 255, as said below
- shuffle_key: int32 [2048], P(('gx', 'gy', 'gz')), may hold values from 0 to 2047, each once
- lengths: int32 [64], replicated, may hold values from 1 to 4096
- gain: float32 [2048], replicated, may hold values from 0.1 to 1.9
Outputs:
- packed: bfloat16 [4096, 128, 2048], P(('gx', 'gy', 'gz'))
The draws below stay inside these ranges and needn't reach their ends.
Inputs may be any that keep to these rules, and one draw needn't show every extreme that they name: `dest_device`: device numbers are ((gx * 4) + gy) * 16 + gz. A device receives at most 16 tiles, and in every draw some devices receive exactly 16. The 16 devices sharing gx and gy send at most one tile to any one device and exactly 8 tiles to the devices of each gz index. Of one device's tiles at most 1 go to devices of one gz index, and some device reaches that.
All inputs are finite; a program needn't handle non-finite values.
Results may differ from the reference program's by a relative error of at most 0.001.
Values may be sent and summed in bfloat16 or wider, within the bound.
No kernel may reach another device: no remote copies, remote signals or barrier semaphores. Data moves between devices by JAX's collectives and lax.ppermute only.
A program may use at most 128 MiB of HBM per device.

```python
import jax
import jax.numpy as jnp
from jax import lax

D = 2048
TILE = 128
TILES_SEQ = 32
TILES_DEV = 8
DEPTH = 16
GROUPS = 16
CAP = 16
TILES = 2048
SEQ_LEN = 4096
SEQS = 64


def draw_dest_device(key, part):
    k_amount, k_label, k_column, k_shift = jax.random.split(key, 4)
    half = GROUPS // 2
    amount = jax.random.randint(k_amount, (DEPTH, half), 0, TILES_DEV + 1)
    amount = amount.at[:, 0].set(TILES_DEV)
    loads = jnp.concatenate([TILES_DEV + amount, TILES_DEV - amount], axis=1)
    labels = jax.vmap(lambda k: jax.random.permutation(k, GROUPS))(jax.random.split(k_label, DEPTH))
    columns = jax.vmap(lambda k: jax.random.permutation(k, GROUPS))(jax.random.split(k_column, DEPTH))
    shift = jax.random.randint(k_shift, (GROUPS,), 0, DEPTH)
    ends = jnp.cumsum(loads, axis=1)
    group = jnp.arange(GROUPS)[:, None, None]
    height = jnp.arange(DEPTH)[None, :, None]
    local = jnp.arange(TILES_DEV)[None, None, :]
    within = height * TILES_DEV + local
    target_z = (within + shift[:, None, None]) % DEPTH
    order = within // DEPTH
    column = columns[target_z, group]
    spot = column + GROUPS * order
    label_index = jnp.sum((spot[..., None] >= ends[target_z]).astype(jnp.int32), axis=-1)
    target_group = labels[target_z, label_index]
    return (target_group * DEPTH + target_z).reshape(-1).astype(jnp.int32)


def set_ends(array, rng, low, largest):
    place = [jax.random.randint(jax.random.fold_in(rng, axis), (), 0, length) for axis, length in enumerate(array.shape)]
    longest = array.shape.index(max(array.shape))
    beside = place[:longest] + [(place[longest] + 1) % array.shape[longest]] + place[longest + 1:]
    return array.at[tuple(place)].set(low).at[tuple(beside)].set(largest)


def steps_of(stream_key, dims, cuts, least, largest):
    level = 1.0
    for dim, shards_of in cuts:
        draws = jax.random.uniform(jax.random.fold_in(jax.random.fold_in(stream_key, 6), dim), (shards_of,), jnp.float32, least / len(cuts), largest / len(cuts))
        level = level * jnp.repeat(jnp.exp(draws), dims[dim] // shards_of).reshape((-1,) + (1,) * (len(dims) - 1 - dim))
    return level


def centred(own_key, dims, scale, most, shards=(), kind=jnp.bfloat16):
    result = jax.random.normal(own_key, dims, jnp.float32) * scale
    if len(shards) > 0:
        result = steps_of(own_key, dims, shards, -0.22, 0.18) * result
    return jnp.clip(result, min=-most, max=most).astype(kind)


def setup_inputs(seed: int = 0) -> dict:
    streams_of = jax.random.split(jax.random.key(seed), 6)
    embeds = centred(streams_of[0], (TILES, TILE, D), 1.0, 6.0, ((0, 256),))
    dest_device = draw_dest_device(jax.random.fold_in(streams_of[5], 71), 0)
    shuffle_key = jax.random.permutation(streams_of[2], TILES).astype(jnp.int32)
    lengths = set_ends(jax.random.randint(streams_of[3], (SEQS,), 1, SEQ_LEN + 1), jax.random.fold_in(streams_of[3], 1), 1, SEQ_LEN).astype(jnp.int32)
    gain = jnp.clip(1.0 + 0.18 * jax.random.normal(streams_of[4], (D,), jnp.float32), 0.1, 1.9)
    return {"embeds": embeds, "dest_device": dest_device, "shuffle_key": shuffle_key, "lengths": lengths, "gain": gain}


def normalize(rows, tile_ids, lengths, gain):
    values = rows.astype(jnp.float32)
    meansq = lax.optimization_barrier(jnp.mean(values * values, axis=-1, keepdims=True))
    scaled = values * lax.rsqrt(jnp.maximum(meansq, 0.25)) * gain.astype(jnp.float32)
    limit = lengths[tile_ids // TILES_SEQ]
    position = (tile_ids % TILES_SEQ)[:, None] * TILE + jnp.arange(TILE, dtype=jnp.int32)[None, :]
    keep = position < limit[:, None]
    return jnp.where(keep[:, :, None], scaled, 0.0).astype(jnp.bfloat16)

def reference(embeds, dest_device, shuffle_key, lengths, gain):
    tile_ids = jnp.arange(TILES, dtype=jnp.int32)
    normed = normalize(embeds, tile_ids, lengths, gain)
    same = dest_device[:, None] == dest_device[None, :]
    earlier = shuffle_key[None, :] < shuffle_key[:, None]
    rank = lax.optimization_barrier(jnp.sum((same & earlier).astype(jnp.int32), axis=1)).astype(jnp.int32)
    slots = (dest_device * CAP + rank).astype(jnp.int32)
    packed = jnp.zeros((GROUPS * DEPTH * CAP, TILE, D), jnp.bfloat16)
    return packed.at[slots].set(normed)
```

```python
import jax
import jax.numpy as jnp
from jax import lax
from jax.experimental import pallas as pl
from jax.experimental.pallas import tpu as pltpu
from jax.sharding import PartitionSpec as P


TILES_SEQ = 32
CHUNKS = (48, 32, 24, 24)
RESIDENT_ROWS = 24
SHIFT_ORDER = (4, 3, 5, 2, 6, 1, 7, 0)


ANY = pl.BlockSpec(memory_space=pl.ANY)
SMEM = pl.BlockSpec(memory_space=pltpu.SMEM)
VMEM = pl.BlockSpec(memory_space=pltpu.VMEM)


def each(count, fn):
    lax.fori_loop(0, count, lambda i, carry: (fn(i), carry)[1], 0)


def shift_order(depth):
    pairs = depth // 2
    return SHIFT_ORDER if pairs == 8 else tuple(range(1, pairs)) + (0,)


def shift_pairs(depth, shift):
    return [(i, (i + 2 * shift) % depth) for i in range(depth)]


def label_first(dest, key, depth):
    def kernel(dest_ref, key_ref, out_ref):
        def clear(s):
            out_ref[s, 0, 0] = -1

        each(depth, clear)

        def note(t):
            peer = lax.rem(dest_ref[t], depth)
            out_ref[peer, 0, 0] = dest_ref[t]
            out_ref[peer, 0, 1] = key_ref[t]

        each(dest.shape[0], note)

    return pl.pallas_call(
        kernel,
        in_specs=[SMEM, SMEM],
        out_specs=SMEM,
        out_shape=jax.ShapeDtypeStruct((depth, 1, 128), jnp.int32),
    )(dest, key)


def label_second(meta, depth, groups):
    def kernel(meta_ref, out_ref):
        def clear(g):
            out_ref[g, 0, 0] = -1

        each(groups, clear)

        def note(h):
            @pl.when(meta_ref[h, 0, 0] >= 0)
            def _():
                out_ref[meta_ref[h, 0, 0] // depth, 0, 0] = meta_ref[h, 0, 1]

        each(depth, note)

    return pl.pallas_call(
        kernel,
        in_specs=[SMEM],
        out_specs=SMEM,
        out_shape=jax.ShapeDtypeStruct((groups, 1, 128), jnp.int32),
    )(meta)


def pack_first(embeds, twin, dest, twin_dest, lengths, gain, start, rows, depth, groups_y):
    tiles, tile_rows, width = embeds.shape
    order = shift_order(depth)
    pairs = depth // 2

    def kernel(dest_ref, twin_dest_ref, len_ref, x_ref, twin_ref, gain_ref, *rest):
        outs = rest[:pairs]
        xin, y, source, sem_in, sem_out = rest[pairs:]
        gz = lax.axis_index("gz")
        core = lax.rem(gz, 2)
        chip = gz // 2
        group = lax.axis_index("gx") * groups_y + lax.axis_index("gy")

        def clear(s):
            source[s] = -1

        each(depth, clear)

        def copy_in(refs, t, slot):
            return pltpu.make_async_copy(
                refs.at[t, pl.ds(start, rows)], xin.at[slot], sem_in.at[slot]
            )

        def note(dests, refs, from_core):
            def one(t):
                peer = lax.rem(dests[t], depth)

                @pl.when(lax.rem(peer, 2) == core)
                def _():
                    slot = lax.rem(peer // 2 - chip + pairs, pairs) * 2 + from_core
                    source[slot] = t
                    copy_in(refs, t, slot).start()

            each(tiles, one)

        note(dest_ref, x_ref, core)
        note(twin_dest_ref, twin_ref, 1 - core)

        def compute(slot):
            t = source[slot]

            @pl.when(t >= 0)
            def _():
                copy_in(x_ref, t, slot).wait()
                from_core = lax.rem(slot, 2)
                tile = (group * depth + chip * 2 + from_core) * tiles + t
                limit = len_ref[tile // TILES_SEQ]
                values = xin[slot].astype(jnp.float32)
                meansq = jnp.sum(values * values, axis=-1, keepdims=True) * (1.0 / width)
                scaled = values * lax.rsqrt(jnp.maximum(meansq, 0.25)) * gain_ref[...]
                row = lax.broadcasted_iota(jnp.int32, (rows, 1), 0)
                keep = lax.rem(tile, TILES_SEQ) * tile_rows + start + row < limit
                y[slot] = jnp.where(keep, scaled, 0.0).astype(y.dtype)

        each(depth, compute)

        def copy_out(s, from_core):
            slot = order[s] * 2 + from_core
            return pltpu.make_async_copy(y.at[slot], outs[s].at[from_core], sem_out.at[slot])

        where = [(s, from_core) for s in range(pairs) for from_core in range(2)]
        for s, from_core in where:
            valid = source[order[s] * 2 + from_core] >= 0
            pl.when(valid)(lambda s=s, from_core=from_core: copy_out(s, from_core).start())
        for s, from_core in where:
            valid = source[order[s] * 2 + from_core] >= 0
            pl.when(valid)(lambda s=s, from_core=from_core: copy_out(s, from_core).wait())

    return pl.pallas_call(
        kernel,
        in_specs=[SMEM, SMEM, SMEM, ANY, ANY, VMEM],
        out_specs=[ANY] * pairs,
        out_shape=[jax.ShapeDtypeStruct((2, rows, width), embeds.dtype)] * pairs,
        scratch_shapes=[
            pltpu.VMEM((depth, rows, width), embeds.dtype),
            pltpu.VMEM((depth, rows, width), embeds.dtype),
            pltpu.SMEM((depth,), jnp.int32),
            pltpu.SemaphoreType.DMA((depth,)),
            pltpu.SemaphoreType.DMA((depth,)),
        ],
    )(dest, twin_dest, lengths, embeds, twin, gain.reshape(1, width))


def pack_second(arrived, meta, depth, groups):
    _, rows, width = arrived[0].shape
    resident = rows <= RESIDENT_ROWS
    order = shift_order(depth)
    pairs = depth // 2

    def kernel(meta_ref, *rest):
        ins = rest[:pairs]
        if resident:
            out_ref, sem_out = rest[pairs:]
        else:
            out_ref, held, sem_in, sem_out = rest[pairs:]
        chip = lax.axis_index("gz") // 2

        dests = []
        for s in range(pairs):
            for from_core in range(2):
                peer = lax.rem(chip - order[s] + pairs, pairs) * 2 + from_core
                dests.append(meta_ref[peer, 0, 0])

        def inward(n):
            return pltpu.make_async_copy(ins[n // 2].at[n % 2], held.at[n], sem_in.at[n])

        def outward(n):
            here = ins[n // 2].at[n % 2] if resident else held.at[n]
            return pltpu.make_async_copy(here, out_ref.at[dests[n] // depth], sem_out.at[n])

        if not resident:
            for n in range(depth):
                pl.when(dests[n] >= 0)(lambda n=n: inward(n).start())
        for n in range(depth):

            @pl.when(dests[n] >= 0)
            def _(n=n):
                if not resident:
                    inward(n).wait()
                outward(n).start()

        for n in range(depth):
            pl.when(dests[n] >= 0)(lambda n=n: outward(n).wait())

    scratch = []
    if not resident:
        scratch = [
            pltpu.VMEM((depth, rows, width), arrived[0].dtype),
            pltpu.SemaphoreType.DMA((depth,)),
        ]
    return pl.pallas_call(
        kernel,
        in_specs=[SMEM] + [VMEM if resident else ANY] * pairs,
        out_specs=ANY,
        out_shape=jax.ShapeDtypeStruct((groups, rows, width), arrived[0].dtype),
        scratch_shapes=scratch + [pltpu.SemaphoreType.DMA((depth,))],
    )(meta, *arrived)


def unpack(arrived, meta, packed, start, tile_rows, cap):
    groups, rows, width = arrived.shape
    first = packed is None
    resident = rows <= RESIDENT_ROWS and not first

    def kernel(meta_ref, in_ref, *rest):
        if first:
            out_ref, held, sem_in, sem_out, zeros, sem_zero = rest
        elif resident:
            _, out_ref, sem_out = rest
        else:
            _, out_ref, held, sem_in, sem_out = rest
        keys = [meta_ref[g, 0, 0] for g in range(groups)]

        def inward(g):
            return pltpu.make_async_copy(in_ref.at[g], held.at[g], sem_in.at[g])

        if not resident:
            for g in range(groups):
                pl.when(keys[g] >= 0)(lambda g=g: inward(g).start())
        ranks = []
        for g in range(groups):
            rank = jnp.int32(0)
            for u in range(groups):
                if u != g:
                    rank = rank + ((keys[u] >= 0) & (keys[u] < keys[g])).astype(jnp.int32)
            ranks.append(rank)
        if first:
            count = jnp.int32(0)
            for g in range(groups):
                count = count + (keys[g] >= 0).astype(jnp.int32)
            zeros[...] = jnp.zeros(zeros.shape, zeros.dtype)

            def fill(s):
                return pltpu.make_async_copy(zeros, out_ref.at[s], sem_zero.at[s])

            each(cap, lambda s: pl.when(s >= count)(lambda: fill(s).start()))

        def outward(g):
            here = in_ref if resident else held
            return pltpu.make_async_copy(
                here.at[g], out_ref.at[ranks[g], pl.ds(start, rows)], sem_out.at[g]
            )

        for g in range(groups):

            @pl.when(keys[g] >= 0)
            def _(g=g):
                if not resident:
                    inward(g).wait()
                outward(g).start()

        for g in range(groups):
            pl.when(keys[g] >= 0)(lambda g=g: outward(g).wait())
        if first:
            each(cap, lambda s: pl.when(s >= count)(lambda: fill(s).wait()))

    scratch = [pltpu.SemaphoreType.DMA((groups,))]
    if not resident:
        scratch = [
            pltpu.VMEM((groups, rows, width), arrived.dtype),
            pltpu.SemaphoreType.DMA((groups,)),
        ] + scratch
    if first:
        scratch += [
            pltpu.VMEM((tile_rows, width), arrived.dtype),
            pltpu.SemaphoreType.DMA((cap,)),
        ]
    return pl.pallas_call(
        kernel,
        in_specs=[SMEM, VMEM if resident else ANY] + ([] if first else [ANY]),
        out_specs=ANY,
        out_shape=jax.ShapeDtypeStruct((cap, tile_rows, width), arrived.dtype),
        scratch_shapes=scratch,
        input_output_aliases={} if first else {2: 0},
    )(meta, arrived, *(() if first else (packed,)))


def shards(embeds, dest_device, shuffle_key, lengths, gain):
    tiles, tile_rows, _ = embeds.shape
    depth = lax.axis_size("gz")
    groups_y = lax.axis_size("gy")
    groups = lax.axis_size("gx") * groups_y
    chunks = CHUNKS if sum(CHUNKS) == tile_rows else (tile_rows,)
    starts = [sum(chunks[:c]) for c in range(len(chunks))]

    partner = [(i, i ^ 1) for i in range(depth)]
    twin = lax.ppermute(embeds, "gz", partner)
    twin_dest = lax.ppermute(dest_device, "gz", partner)
    meta = label_first(dest_device, shuffle_key, depth)
    meta = lax.all_to_all(meta, "gz", split_axis=0, concat_axis=0, tiled=True)
    last_meta = label_second(meta, depth, groups)
    last_meta = lax.all_to_all(
        last_meta, ("gx", "gy"), split_axis=0, concat_axis=0, tiled=True
    )
    meta, last_meta = lax.optimization_barrier((meta, last_meta))

    crossing = []
    for start, rows in zip(starts, chunks):
        sent = pack_first(
            embeds, twin, dest_device, twin_dest, lengths, gain, start, rows, depth, groups_y
        )
        crossing.append(
            [
                lax.ppermute(slots, "gz", shift_pairs(depth, shift)) if shift else slots
                for slots, shift in zip(sent, shift_order(depth))
            ]
        )

    packed = landed = None
    for c, (start, rows) in enumerate(zip(starts, chunks)):
        sent = pack_second(crossing[c], meta, depth, groups)
        if c > 0:
            sent, landed = lax.optimization_barrier((sent, landed))
            packed = unpack(
                landed, last_meta, packed, starts[c - 1], tile_rows, 2 * tiles
            )
        landed = lax.all_to_all(sent, ("gx", "gy"), split_axis=0, concat_axis=0, tiled=True)
    return unpack(landed, last_meta, packed, starts[-1], tile_rows, 2 * tiles)


def solution(mesh):
    return jax.shard_map(
        shards,
        mesh=mesh,
        in_specs=(
            P(("gx", "gy", "gz"), None, None),
            P(("gx", "gy", "gz")),
            P(("gx", "gy", "gz")),
            P(),
            P(),
        ),
        out_specs=P(("gx", "gy", "gz"), None, None),
        check_vma=False,
    )
```

```python
import jax
import jax.numpy as jnp
from jax import lax
from jax.experimental import pallas as pl
from jax.experimental.pallas import tpu as pltpu
from jax.sharding import PartitionSpec as P


TILES_SEQ = 32
CHUNKS = (56, 32, 24, 16)
SHIFT_ORDER = (4, 3, 5, 2, 6, 1, 7, 0)


ANY = pl.BlockSpec(memory_space=pl.ANY)
SMEM = pl.BlockSpec(memory_space=pltpu.SMEM)
VMEM = pl.BlockSpec(memory_space=pltpu.VMEM)


def each(count, fn):
    lax.fori_loop(0, count, lambda i, carry: (fn(i), carry)[1], 0)


def shift_order(depth):
    pairs = depth // 2
    return SHIFT_ORDER if pairs == 8 else tuple(range(1, pairs)) + (0,)


def shift_pairs(depth, shift):
    return [(i, (i + 2 * shift) % depth) for i in range(depth)]


def label_first(dest, key, depth):
    def kernel(dest_ref, key_ref, out_ref):
        def clear(s):
            out_ref[s, 0, 0] = -1

        each(depth, clear)

        def note(t):
            peer = lax.rem(dest_ref[t], depth)
            out_ref[peer, 0, 0] = dest_ref[t]
            out_ref[peer, 0, 1] = key_ref[t]

        each(dest.shape[0], note)

    return pl.pallas_call(
        kernel,
        in_specs=[SMEM, SMEM],
        out_specs=SMEM,
        out_shape=jax.ShapeDtypeStruct((depth, 1, 128), jnp.int32),
    )(dest, key)


def label_second(meta, depth, groups):
    def kernel(meta_ref, out_ref):
        def clear(g):
            out_ref[g, 0, 0] = -1

        each(groups, clear)

        def note(h):
            @pl.when(meta_ref[h, 0, 0] >= 0)
            def _():
                out_ref[meta_ref[h, 0, 0] // depth, 0, 0] = meta_ref[h, 0, 1]

        each(depth, note)

    return pl.pallas_call(
        kernel,
        in_specs=[SMEM],
        out_specs=SMEM,
        out_shape=jax.ShapeDtypeStruct((groups, 1, 128), jnp.int32),
    )(meta)


def pack_first(sources, lengths, gain, start, rows, depth, groups_y):
    tiles, tile_rows, width = sources[0][0].shape
    count = len(sources)
    order = shift_order(depth)
    pairs = depth // 2
    slot_shape = (rows, width) if count == 1 else (count, rows, width)

    def kernel(*refs):
        dests = refs[:count]
        inputs = refs[count : 2 * count]
        len_ref, gain_ref = refs[2 * count : 2 * count + 2]
        outs = refs[2 * count + 2 : 2 * count + 2 + pairs]
        xin, y, source, sem_in, sem_out = refs[2 * count + 2 + pairs :]
        gz = lax.axis_index("gz")
        core = lax.rem(gz, 2)
        chip = gz // 2
        group = lax.axis_index("gx") * groups_y + lax.axis_index("gy")

        def clear(s):
            source[s] = -1

        each(depth, clear)

        def copy_in(n, t, slot):
            return pltpu.make_async_copy(
                inputs[n].at[t, pl.ds(start, rows)], xin.at[slot], sem_in.at[slot]
            )

        for n in range(count):
            from_core = core if sources[n][2] == 0 else 1 - core

            def note(t, n=n, from_core=from_core):
                peer = lax.rem(dests[n][t], depth)

                @pl.when(lax.rem(peer, 2) == core)
                def _():
                    slot = lax.rem(peer // 2 - chip + pairs, pairs) * 2 + from_core
                    source[slot] = t
                    copy_in(n, t, slot).start()

            each(tiles, note)

        def compute(slot):
            t = source[slot]

            @pl.when(t >= 0)
            def _():
                copy_in(0, t, slot).wait()
                tile = (group * depth + chip * 2 + lax.rem(slot, 2)) * tiles + t
                limit = len_ref[tile // TILES_SEQ]
                values = xin[slot].astype(jnp.float32)
                meansq = jnp.sum(values * values, axis=-1, keepdims=True) * (1.0 / width)
                scaled = values * lax.rsqrt(jnp.maximum(meansq, 0.25)) * gain_ref[...]
                row = lax.broadcasted_iota(jnp.int32, (rows, 1), 0)
                keep = lax.rem(tile, TILES_SEQ) * tile_rows + start + row < limit
                y[slot] = jnp.where(keep, scaled, 0.0).astype(y.dtype)

        each(depth, compute)

        def copy_out(s, n):
            if count == 1:
                slot = order[s] * 2 + (core if sources[0][2] == 0 else 1 - core)
                return slot, lambda: pltpu.make_async_copy(y.at[slot], outs[s], sem_out.at[slot])
            slot = order[s] * 2 + n
            return slot, lambda: pltpu.make_async_copy(y.at[slot], outs[s].at[n], sem_out.at[slot])

        where = [(s, n) for s in range(pairs) for n in range(count)]
        for s, n in where:
            slot, copy = copy_out(s, n)
            pl.when(source[slot] >= 0)(lambda copy=copy: copy().start())
        for s, n in where:
            slot, copy = copy_out(s, n)
            pl.when(source[slot] >= 0)(lambda copy=copy: copy().wait())

    dtype = sources[0][0].dtype
    return pl.pallas_call(
        kernel,
        in_specs=[SMEM] * count + [ANY] * count + [SMEM, VMEM],
        out_specs=[ANY] * pairs,
        out_shape=[jax.ShapeDtypeStruct(slot_shape, dtype)] * pairs,
        scratch_shapes=[
            pltpu.VMEM((depth, rows, width), dtype),
            pltpu.VMEM((depth, rows, width), dtype),
            pltpu.SMEM((depth,), jnp.int32),
            pltpu.SemaphoreType.DMA((depth,)),
            pltpu.SemaphoreType.DMA((depth,)),
        ],
    )(*(d for _, d, _ in sources), *(x for x, _, _ in sources), lengths, gain.reshape(1, width))


def pack_second(arrived, meta, depth, groups, resident):
    rows, width = arrived[0].shape[-2:]
    order = shift_order(depth)
    pairs = depth // 2
    count = len(arrived)

    def kernel(meta_ref, *rest):
        ins = rest[:count]
        if resident:
            out_ref, sem_out = rest[count:]
        else:
            out_ref, held, sem_in, sem_out = rest[count:]
        gz = lax.axis_index("gz")
        chip = gz // 2
        core = lax.rem(gz, 2)
        if count == pairs:
            pieces = [ins[n // 2].at[n % 2] for n in range(depth)]
        else:
            pieces = [ins[n // 2 + pairs * (n % 2)] for n in range(depth)]

        dests = []
        for s in range(pairs):
            for from_core in range(2):
                sender = from_core if count == pairs else lax.rem(core + from_core, 2)
                peer = lax.rem(chip - order[s] + pairs, pairs) * 2 + sender
                dests.append(meta_ref[peer, 0, 0])

        def inward(n):
            return pltpu.make_async_copy(pieces[n], held.at[n], sem_in.at[n])

        def outward(n):
            here = pieces[n] if resident else held.at[n]
            return pltpu.make_async_copy(here, out_ref.at[dests[n] // depth], sem_out.at[n])

        if not resident:
            for n in range(depth):
                pl.when(dests[n] >= 0)(lambda n=n: inward(n).start())
        for n in range(depth):

            @pl.when(dests[n] >= 0)
            def _(n=n):
                if not resident:
                    inward(n).wait()
                outward(n).start()

        for n in range(depth):
            pl.when(dests[n] >= 0)(lambda n=n: outward(n).wait())

    scratch = []
    if not resident:
        scratch = [
            pltpu.VMEM((depth, rows, width), arrived[0].dtype),
            pltpu.SemaphoreType.DMA((depth,)),
        ]
    return pl.pallas_call(
        kernel,
        in_specs=[SMEM] + [VMEM if resident else ANY] * count,
        out_specs=ANY,
        out_shape=jax.ShapeDtypeStruct((groups, rows, width), arrived[0].dtype),
        scratch_shapes=scratch + [pltpu.SemaphoreType.DMA((depth,))],
    )(meta, *arrived)


def unpack(arrived, meta, packed, start, tile_rows, cap, resident=False):
    groups, rows, width = arrived.shape
    first = packed is None

    def kernel(*refs):
        meta_ref, in_ref, *rest = refs if first else refs[1:]
        if first:
            out_ref, held, sem_in, sem_out, zeros, sem_zero = rest
        elif resident:
            out_ref, sem_out = rest
        else:
            out_ref, held, sem_in, sem_out = rest
        keys = [meta_ref[g, 0, 0] for g in range(groups)]

        def inward(g):
            return pltpu.make_async_copy(in_ref.at[g], held.at[g], sem_in.at[g])

        if not resident:
            for g in range(groups):
                pl.when(keys[g] >= 0)(lambda g=g: inward(g).start())
        ranks = []
        for g in range(groups):
            rank = jnp.int32(0)
            for u in range(groups):
                if u != g:
                    rank = rank + ((keys[u] >= 0) & (keys[u] < keys[g])).astype(jnp.int32)
            ranks.append(rank)
        if first:
            count = jnp.int32(0)
            for g in range(groups):
                count = count + (keys[g] >= 0).astype(jnp.int32)
            zeros[...] = jnp.zeros(zeros.shape, zeros.dtype)

            def fill(s):
                return pltpu.make_async_copy(zeros, out_ref.at[s], sem_zero.at[s])

            each(cap, lambda s: pl.when(s >= count)(lambda: fill(s).start()))

        def outward(g):
            here = in_ref if resident else held
            return pltpu.make_async_copy(
                here.at[g], out_ref.at[ranks[g], pl.ds(start, rows)], sem_out.at[g]
            )

        for g in range(groups):

            @pl.when(keys[g] >= 0)
            def _(g=g):
                if not resident:
                    inward(g).wait()
                outward(g).start()

        for g in range(groups):
            pl.when(keys[g] >= 0)(lambda g=g: outward(g).wait())
        if first:
            each(cap, lambda s: pl.when(s >= count)(lambda: fill(s).wait()))

    scratch = [pltpu.SemaphoreType.DMA((groups,))]
    if not resident:
        scratch = [
            pltpu.VMEM((groups, rows, width), arrived.dtype),
            pltpu.SemaphoreType.DMA((groups,)),
        ] + scratch
    if first:
        scratch += [
            pltpu.VMEM((tile_rows, width), arrived.dtype),
            pltpu.SemaphoreType.DMA((cap,)),
        ]
    return pl.pallas_call(
        kernel,
        in_specs=([] if first else [ANY]) + [SMEM, VMEM if resident else ANY],
        out_specs=ANY,
        out_shape=jax.ShapeDtypeStruct((cap, tile_rows, width), arrived.dtype),
        scratch_shapes=scratch,
        input_output_aliases={} if first else {0: 0},
    )(*(() if first else (packed,)), meta, arrived)


def shards(embeds, dest_device, shuffle_key, lengths, gain):
    tiles, tile_rows, _ = embeds.shape
    depth = lax.axis_size("gz")
    groups_y = lax.axis_size("gy")
    groups = lax.axis_size("gx") * groups_y
    chunks = CHUNKS if sum(CHUNKS) == tile_rows else (tile_rows,)
    starts = [sum(chunks[:c]) for c in range(len(chunks))]

    partner = [(i, i ^ 1) for i in range(depth)]
    twin = lax.ppermute(embeds, "gz", partner)
    twin_dest = lax.ppermute(dest_device, "gz", partner)
    meta = label_first(dest_device, shuffle_key, depth)
    meta = lax.all_to_all(meta, "gz", split_axis=0, concat_axis=0, tiled=True)
    last_meta = label_second(meta, depth, groups)
    last_meta = lax.all_to_all(
        last_meta, ("gx", "gy"), split_axis=0, concat_axis=0, tiled=True
    )
    meta, last_meta = lax.optimization_barrier((meta, last_meta))

    own, other = (embeds, dest_device, 0), (twin, twin_dest, 1)
    units = [((own,), 0), ((other,), 0)] + [((own, other), c) for c in range(1, len(chunks))]
    crossing = [[] for _ in chunks]
    for sources, c in units:
        sent = pack_first(sources, lengths, gain, starts[c], chunks[c], depth, groups_y)
        crossing[c] += [
            lax.ppermute(slots, "gz", shift_pairs(depth, shift)) if shift else slots
            for slots, shift in zip(sent, shift_order(depth))
        ]

    packed = landed = None
    for c, (start, rows) in enumerate(zip(starts, chunks)):
        resident = c > 0 and c == len(chunks) - 1
        if resident:
            crossing[c] = [
                pltpu.with_memory_space_constraint(slots, pltpu.VMEM) for slots in crossing[c]
            ]
        sent = pack_second(crossing[c], meta, depth, groups, resident)
        if c > 0:
            sent, landed = lax.optimization_barrier((sent, landed))
            packed = unpack(
                landed, last_meta, packed, starts[c - 1], tile_rows, 2 * tiles
            )
        landed = lax.all_to_all(sent, ("gx", "gy"), split_axis=0, concat_axis=0, tiled=True)
    if resident:
        landed = pltpu.with_memory_space_constraint(landed, pltpu.VMEM)
    return unpack(landed, last_meta, packed, starts[-1], tile_rows, 2 * tiles, resident)


def solution(mesh):
    return jax.shard_map(
        shards,
        mesh=mesh,
        in_specs=(
            P(("gx", "gy", "gz"), None, None),
            P(("gx", "gy", "gz")),
            P(("gx", "gy", "gz")),
            P(),
            P(),
        ),
        out_specs=P(("gx", "gy", "gz"), None, None),
        check_vma=False,
    )
```

```python
import jax
import jax.numpy as jnp
from jax import lax
from jax.experimental import pallas as pl
from jax.experimental.pallas import tpu as pltpu
from jax.sharding import PartitionSpec as P


TILES_SEQ = 32
CHUNKS = (48, 40, 24, 16)
SHIFT_ORDER = (4, 3, 5, 2, 6, 1, 7, 0)


ANY = pl.BlockSpec(memory_space=pl.ANY)
SMEM = pl.BlockSpec(memory_space=pltpu.SMEM)
VMEM = pl.BlockSpec(memory_space=pltpu.VMEM)


def each(count, fn):
    lax.fori_loop(0, count, lambda i, carry: (fn(i), carry)[1], 0)


def shift_order(depth):
    pairs = depth // 2
    return SHIFT_ORDER if pairs == 8 else tuple(range(1, pairs)) + (0,)


def shift_pairs(depth, shift):
    return [(i, (i + 2 * shift) % depth) for i in range(depth)]


def label_first(dest, key, depth):
    def kernel(dest_ref, key_ref, out_ref):
        def clear(s):
            out_ref[s, 0, 0] = -1

        each(depth, clear)

        def note(t):
            peer = lax.rem(dest_ref[t], depth)
            out_ref[peer, 0, 0] = dest_ref[t]
            out_ref[peer, 0, 1] = key_ref[t]

        each(dest.shape[0], note)

    return pl.pallas_call(
        kernel,
        in_specs=[SMEM, SMEM],
        out_specs=SMEM,
        out_shape=jax.ShapeDtypeStruct((depth, 1, 128), jnp.int32),
    )(dest, key)


def label_second(meta, depth, groups):
    def kernel(meta_ref, out_ref):
        def clear(g):
            out_ref[g, 0, 0] = -1

        each(groups, clear)

        def note(h):
            @pl.when(meta_ref[h, 0, 0] >= 0)
            def _():
                out_ref[meta_ref[h, 0, 0] // depth, 0, 0] = meta_ref[h, 0, 1]

        each(depth, note)

    return pl.pallas_call(
        kernel,
        in_specs=[SMEM],
        out_specs=SMEM,
        out_shape=jax.ShapeDtypeStruct((groups, 1, 128), jnp.int32),
    )(meta)


def pack_first(sources, lengths, gain, start, rows, depth, groups_y):
    tiles, tile_rows, width = sources[0][0].shape
    count = len(sources)
    order = shift_order(depth)
    pairs = depth // 2
    slot_shape = (rows, width) if count == 1 else (count, rows, width)

    def kernel(*refs):
        dests = refs[:count]
        inputs = refs[count : 2 * count]
        len_ref, gain_ref = refs[2 * count : 2 * count + 2]
        outs = refs[2 * count + 2 : 2 * count + 2 + pairs]
        xin, y, source, sem_in, sem_out = refs[2 * count + 2 + pairs :]
        gz = lax.axis_index("gz")
        core = lax.rem(gz, 2)
        chip = gz // 2
        group = lax.axis_index("gx") * groups_y + lax.axis_index("gy")

        def clear(s):
            source[s] = -1

        each(depth, clear)

        def copy_in(n, t, slot):
            return pltpu.make_async_copy(
                inputs[n].at[t, pl.ds(start, rows)], xin.at[slot], sem_in.at[slot]
            )

        for n in range(count):
            from_core = core if sources[n][2] == 0 else 1 - core

            def note(t, n=n, from_core=from_core):
                peer = lax.rem(dests[n][t], depth)

                @pl.when(lax.rem(peer, 2) == core)
                def _():
                    slot = lax.rem(peer // 2 - chip + pairs, pairs) * 2 + from_core
                    source[slot] = t
                    copy_in(n, t, slot).start()

            each(tiles, note)

        def compute(slot):
            t = source[slot]

            @pl.when(t >= 0)
            def _():
                copy_in(0, t, slot).wait()
                tile = (group * depth + chip * 2 + lax.rem(slot, 2)) * tiles + t
                limit = len_ref[tile // TILES_SEQ]
                values = xin[slot].astype(jnp.float32)
                meansq = jnp.sum(values * values, axis=-1, keepdims=True) * (1.0 / width)
                scaled = values * lax.rsqrt(jnp.maximum(meansq, 0.25)) * gain_ref[...]
                row = lax.broadcasted_iota(jnp.int32, (rows, 1), 0)
                keep = lax.rem(tile, TILES_SEQ) * tile_rows + start + row < limit
                y[slot] = jnp.where(keep, scaled, 0.0).astype(y.dtype)

        each(depth, compute)

        def copy_out(s, n):
            if count == 1:
                slot = order[s] * 2 + (core if sources[0][2] == 0 else 1 - core)
                return slot, lambda: pltpu.make_async_copy(y.at[slot], outs[s], sem_out.at[slot])
            slot = order[s] * 2 + n
            return slot, lambda: pltpu.make_async_copy(y.at[slot], outs[s].at[n], sem_out.at[slot])

        where = [(s, n) for s in range(pairs) for n in range(count)]
        for s, n in where:
            slot, copy = copy_out(s, n)
            pl.when(source[slot] >= 0)(lambda copy=copy: copy().start())

        def finish(slot):
            @pl.when(source[slot] >= 0)
            def _():
                out = outs[0] if count == 1 else outs[0].at[0]
                pltpu.make_async_copy(y.at[slot], out, sem_out.at[slot]).wait()

        each(depth, finish)

    dtype = sources[0][0].dtype
    return pl.pallas_call(
        kernel,
        in_specs=[SMEM] * count + [ANY] * count + [SMEM, VMEM],
        out_specs=[ANY] * pairs,
        out_shape=[jax.ShapeDtypeStruct(slot_shape, dtype)] * pairs,
        scratch_shapes=[
            pltpu.VMEM((depth, rows, width), dtype),
            pltpu.VMEM((depth, rows, width), dtype),
            pltpu.SMEM((depth,), jnp.int32),
            pltpu.SemaphoreType.DMA((depth,)),
            pltpu.SemaphoreType.DMA((depth,)),
        ],
    )(*(d for _, d, _ in sources), *(x for x, _, _ in sources), lengths, gain.reshape(1, width))


def pack_second(arrived, meta, depth, groups, resident):
    rows, width = arrived[0].shape[-2:]
    order = shift_order(depth)
    pairs = depth // 2
    count = len(arrived)

    def kernel(meta_ref, *rest):
        ins = rest[:count]
        if resident:
            out_ref, group_of, sem_out = rest[count:]
        else:
            out_ref, group_of, held, sem_in, sem_out = rest[count:]
        gz = lax.axis_index("gz")
        chip = gz // 2
        core = lax.rem(gz, 2)
        if count == pairs:
            pieces = [ins[n // 2].at[n % 2] for n in range(depth)]
        else:
            pieces = [ins[n // 2 + pairs * (n % 2)] for n in range(depth)]

        for n in range(depth):
            sender = n % 2 if count == pairs else lax.rem(core + n % 2, 2)
            peer = lax.rem(chip - order[n // 2] + pairs, pairs) * 2 + sender
            dest = meta_ref[peer, 0, 0]
            group = jnp.maximum(dest, 0) // depth
            group_of[n] = jnp.where(dest >= 0, group, -1)
            if resident:
                copy = lambda n=n, group=group: pltpu.make_async_copy(
                    pieces[n], out_ref.at[group], sem_out.at[n]
                )
            else:
                copy = lambda n=n: pltpu.make_async_copy(pieces[n], held.at[n], sem_in.at[n])
            pl.when(dest >= 0)(lambda copy=copy: copy().start())

        def outward(n):
            here = pieces[0] if resident else held.at[n]
            return pltpu.make_async_copy(here, out_ref.at[group_of[n]], sem_out.at[n])

        def forward(n):
            pltpu.make_async_copy(pieces[0], held.at[n], sem_in.at[n]).wait()
            outward(n).start()

        def valid(fn):
            each(depth, lambda n: pl.when(group_of[n] >= 0)(lambda: fn(n)))

        if not resident:
            valid(forward)
        valid(lambda n: outward(n).wait())

    scratch = []
    if not resident:
        scratch = [
            pltpu.VMEM((depth, rows, width), arrived[0].dtype),
            pltpu.SemaphoreType.DMA((depth,)),
        ]
    return pl.pallas_call(
        kernel,
        in_specs=[SMEM] + [VMEM if resident else ANY] * count,
        out_specs=ANY,
        out_shape=jax.ShapeDtypeStruct((groups, rows, width), arrived[0].dtype),
        scratch_shapes=[pltpu.SMEM((depth,), jnp.int32)]
        + scratch
        + [pltpu.SemaphoreType.DMA((depth,))],
    )(meta, *arrived)


def rank_arrivals(meta, groups):
    def kernel(meta_ref, out_ref):
        keys = [meta_ref[g, 0, 0] for g in range(groups)]
        count = jnp.int32(0)
        for g in range(groups):
            rank = jnp.int32(0)
            for u in range(groups):
                if u != g:
                    rank = rank + ((keys[u] >= 0) & (keys[u] < keys[g])).astype(jnp.int32)
            out_ref[g] = jnp.where(keys[g] >= 0, rank, -1)
            count = count + (keys[g] >= 0).astype(jnp.int32)
        out_ref[groups] = count

    return pl.pallas_call(
        kernel,
        in_specs=[SMEM],
        out_specs=SMEM,
        out_shape=jax.ShapeDtypeStruct((128,), jnp.int32),
    )(meta)


def unpack(arrived, ranks, packed, start, tile_rows, cap, resident=False):
    groups, rows, width = arrived.shape
    first = packed is None

    def kernel(*refs):
        rank_ref, in_ref, *rest = refs if first else refs[1:]
        if first:
            out_ref, held, sem_in, sem_out, zeros, sem_zero = rest
        elif resident:
            out_ref, sem_out = rest
        else:
            out_ref, held, sem_in, sem_out = rest

        def inward(g):
            return pltpu.make_async_copy(in_ref.at[g], held.at[g], sem_in.at[g])

        def outward(g):
            here = in_ref if resident else held
            return pltpu.make_async_copy(
                here.at[g], out_ref.at[rank_ref[g], pl.ds(start, rows)], sem_out.at[g]
            )

        def forward(g):
            if not resident:
                inward(g).wait()
            outward(g).start()

        def valid(fn):
            each(groups, lambda g: pl.when(rank_ref[g] >= 0)(lambda: fn(g)))

        if not resident:
            valid(lambda g: inward(g).start())
        if first:
            count = rank_ref[groups]
            zeros[...] = jnp.zeros(zeros.shape, zeros.dtype)

            def fill(s):
                return pltpu.make_async_copy(zeros, out_ref.at[s], sem_zero.at[s])

            each(cap, lambda s: pl.when(s >= count)(lambda: fill(s).start()))
        valid(forward)
        valid(lambda g: outward(g).wait())
        if first:
            each(cap, lambda s: pl.when(s >= count)(lambda: fill(s).wait()))

    scratch = [pltpu.SemaphoreType.DMA((groups,))]
    if not resident:
        scratch = [
            pltpu.VMEM((groups, rows, width), arrived.dtype),
            pltpu.SemaphoreType.DMA((groups,)),
        ] + scratch
    if first:
        scratch += [
            pltpu.VMEM((tile_rows, width), arrived.dtype),
            pltpu.SemaphoreType.DMA((cap,)),
        ]
    return pl.pallas_call(
        kernel,
        in_specs=([] if first else [ANY]) + [SMEM, VMEM if resident else ANY],
        out_specs=ANY,
        out_shape=jax.ShapeDtypeStruct((cap, tile_rows, width), arrived.dtype),
        scratch_shapes=scratch,
        input_output_aliases={} if first else {0: 0},
    )(*(() if first else (packed,)), ranks, arrived)


def shards(embeds, dest_device, shuffle_key, lengths, gain):
    tiles, tile_rows, _ = embeds.shape
    depth = lax.axis_size("gz")
    groups_y = lax.axis_size("gy")
    groups = lax.axis_size("gx") * groups_y
    chunks = CHUNKS if sum(CHUNKS) == tile_rows else (tile_rows,)
    starts = [sum(chunks[:c]) for c in range(len(chunks))]

    partner = [(i, i ^ 1) for i in range(depth)]
    twin = lax.ppermute(embeds, "gz", partner)
    twin_dest = lax.ppermute(dest_device, "gz", partner)
    meta = label_first(dest_device, shuffle_key, depth)
    meta = lax.all_to_all(meta, "gz", split_axis=0, concat_axis=0, tiled=True)
    last_meta = label_second(meta, depth, groups)
    last_meta = lax.all_to_all(
        last_meta, ("gx", "gy"), split_axis=0, concat_axis=0, tiled=True
    )
    meta, last_meta = lax.optimization_barrier((meta, last_meta))
    ranks = rank_arrivals(last_meta, groups)

    own, other = (embeds, dest_device, 0), (twin, twin_dest, 1)
    units = [((own,), 0), ((other,), 0)] + [((own, other), c) for c in range(1, len(chunks))]
    crossing = [[] for _ in chunks]
    for sources, c in units:
        sent = pack_first(sources, lengths, gain, starts[c], chunks[c], depth, groups_y)
        crossing[c] += [
            lax.ppermute(slots, "gz", shift_pairs(depth, shift)) if shift else slots
            for slots, shift in zip(sent, shift_order(depth))
        ]

    packed = landed = None
    for c, (start, rows) in enumerate(zip(starts, chunks)):
        resident = c > 0 and c == len(chunks) - 1
        if resident:
            crossing[c] = [
                pltpu.with_memory_space_constraint(slots, pltpu.VMEM) for slots in crossing[c]
            ]
        sent = pack_second(crossing[c], meta, depth, groups, resident)
        if c > 0:
            sent, landed = lax.optimization_barrier((sent, landed))
            packed = unpack(
                landed, ranks, packed, starts[c - 1], tile_rows, 2 * tiles
            )
        landed = lax.all_to_all(sent, ("gx", "gy"), split_axis=0, concat_axis=0, tiled=True)
    if resident:
        landed = pltpu.with_memory_space_constraint(landed, pltpu.VMEM)
    return unpack(landed, ranks, packed, starts[-1], tile_rows, 2 * tiles, resident)


def solution(mesh):
    return jax.shard_map(
        shards,
        mesh=mesh,
        in_specs=(
            P(("gx", "gy", "gz"), None, None),
            P(("gx", "gy", "gz")),
            P(("gx", "gy", "gz")),
            P(),
            P(),
        ),
        out_specs=P(("gx", "gy", "gz"), None, None),
        check_vma=False,
    )
```
